256 devices in a mesh: row: 16 (over x_lo, y, core), col: 16 (over z, x_hi).
Axes of the slice: x: 4 (x_hi: 2, x_lo: 2; x = x_hi * 2 + x_lo), y: 4, z: 8, core: 2. Of those that a mesh axis runs over, the one named last changes fastest.
Arguments:
- orbital_factors: bfloat16 [2048, 8, 6144], P(('row', 'col')), may hold values from -0.045166016 to 0.045166016
- occ_energy: bfloat16 [8], replicated, may hold values from -2 to -0.29882812
- virt_energy: bfloat16 [2048], P(('row', 'col')), may hold values from 0.19921875 to 4
Outputs:
- pair_energy: float32 [8, 8], replicated
- virt_share: float32 [2048], P(('row', 'col'))
The draws below stay inside these ranges and needn't reach their ends.
All inputs are finite; a program needn't handle non-finite values.
Results may differ from the reference program's by a relative error of at most 0.0003.
Values may be sent and summed in bfloat16 or wider, within the bound.
A program may use at most 64 MiB of HBM per device.

```python
import jax
import jax.numpy as jnp
from jax import lax

NOCC = 8
V = 2048
NAUX = 6144


def block_levels(key, dims, cuts, low, high):
    def one(position, parts):
        steps = jax.random.uniform(jax.random.fold_in(jax.random.fold_in(key, 6), position), (parts,), jnp.float32, low / len(cuts), high / len(cuts))
        return jnp.repeat(jnp.exp(steps), dims[position] // parts).reshape((-1,) + (1,) * (len(dims) - position - 1))

    level = one(*cuts[0])
    for cut in cuts[1:]:
        level = level * one(*cut)
    return level


def scatter_about(key, extent, spread, reach, pieces=(), kind=jnp.bfloat16):
    gain = block_levels(key, extent, pieces, -0.22, 0.18) if pieces else 1.0
    drawn = jax.random.normal(key, extent, jnp.float32) * spread * gain
    return jnp.minimum(jnp.maximum(drawn, -reach), reach).astype(kind)


def setup_inputs(seed: int = 0) -> dict:
    streams_of = jax.random.split(jax.random.key(seed), 4)
    orbital_factors = scatter_about(streams_of[0], (V, NOCC, NAUX), (0.063 * NAUX ** -0.25), 0.045166016, ((0, 256),))
    occ_energy = jnp.clip(jax.random.uniform(streams_of[1], (NOCC,), jnp.float32, -2.0, -0.29882812), -2.0, -0.29882812).astype(jnp.bfloat16)
    virt_energy = jnp.clip(0.19921875 + 3.8007812 * jax.random.uniform(streams_of[2], (V,), jnp.float32) ** block_levels(streams_of[2], (V,), ((0, 256),), -0.2, 0.2), 0.19921875, 4.0).astype(jnp.bfloat16)
    return {"orbital_factors": orbital_factors, "occ_energy": occ_energy, "virt_energy": virt_energy}


def reference(orbital_factors, occ_energy, virt_energy):
    occupied = occ_energy.astype(jnp.float32)
    virtual = virt_energy.astype(jnp.float32)
    width = min(V, 128)
    count = V // width
    flat = orbital_factors.reshape(V * NOCC, NAUX)
    blocks = orbital_factors.reshape(count, width, NOCC, NAUX)
    block_eps = virtual.reshape(count, width)

    def one_block(packed):
        virt_block, eps_block = packed
        integral = lax.dot_general(virt_block.reshape(width * NOCC, NAUX), flat, (((1,), (1,)), ((), ())), preferred_element_type=jnp.float32)
        integral = integral.reshape(width, NOCC, V, NOCC)
        swapped = jnp.transpose(integral, (0, 3, 2, 1))
        denominator = occupied[None, :, None, None] + occupied[None, None, None, :] - eps_block[:, None, None, None] - virtual[None, None, :, None]
        energy_terms = integral * (2.0 * integral - swapped) / denominator
        return jnp.sum(energy_terms, axis=(0, 2)), jnp.sum(energy_terms, axis=(1, 2, 3))

    pair_parts, virt_parts = lax.map(one_block, (blocks, block_eps))
    return jnp.sum(pair_parts, axis=0), virt_parts.reshape(V)
```

```python
import functools

import jax
import jax.numpy as jnp
import numpy as np
from jax import lax
from jax.experimental import pallas as pl
from jax.experimental.pallas import tpu as pltpu
from jax.sharding import PartitionSpec as P

OFFSETS = (
    (0, 1, 7),
    (0, 3, 7),
    (1, 3, 3),
    (2, 3, 7),
    (0, 0, 7),
    (0, 2, 7),
    (2, 2, 7),
    (1, 0, 0),
    (2, 0, 3),
    (3, 0, 2),
    (2, 0, 2),
    (1, 3, 7),
    (3, 0, 1),
    (0, 0, 1),
    (1, 0, 3),
    (0, 0, 0),
)
COLS = 8
ROW0 = 5
NROW = 11
FIRST = 0
LAST = 5
PLAN = (
    (1, 0, 15, 0, 7), (1, 0, 15, 4, 13), (1, 0, 15, 5, 4), (1, 1, 15, 0, 7), (1, 1, 15, 4, 13), (1, 1, 15, 5, 4),
    (1, 2, 15, 0, 7), (1, 2, 15, 4, 13), (1, 2, 15, 5, 4), (0, 0, 4, 0, 0), (0, 0, 7, 0, 0), (0, 0, 13, 0, 0),
    (1, 0, 4, 2, 0), (1, 0, 4, 3, 1), (1, 0, 13, 1, 12), (1, 3, 15, 0, 7), (1, 3, 15, 4, 13), (1, 3, 15, 5, 4),
    (0, 1, 4, 0, 0), (0, 1, 7, 0, 0), (0, 1, 13, 0, 0), (1, 1, 4, 2, 0), (1, 1, 4, 3, 1), (1, 1, 13, 1, 12),
    (1, 4, 15, 5, 4), (0, 0, 0, 0, 0), (0, 0, 1, 0, 0), (0, 0, 12, 0, 0), (1, 0, 0, 2, 5), (1, 0, 1, 0, 11),
    (1, 0, 12, 4, 9), (0, 2, 4, 0, 0), (0, 2, 7, 0, 0), (0, 2, 13, 0, 0), (1, 2, 4, 2, 0), (1, 2, 4, 3, 1),
    (1, 2, 13, 1, 12), (1, 5, 15, 5, 4), (0, 1, 0, 0, 0), (0, 1, 1, 0, 0), (0, 1, 12, 0, 0), (1, 1, 1, 0, 11),
    (1, 1, 12, 4, 9), (1, 1, 0, 2, 5), (0, 3, 4, 0, 0), (0, 3, 7, 0, 0), (0, 3, 13, 0, 0), (1, 3, 4, 3, 1),
    (1, 3, 13, 1, 12), (1, 4, 15, 4, 13), (0, 0, 5, 0, 0), (0, 2, 1, 0, 0), (0, 2, 12, 0, 0), (1, 3, 4, 2, 0),
    (0, 0, 9, 0, 0), (0, 0, 11, 0, 0), (0, 4, 4, 0, 0), (1, 0, 9, 1, 10), (1, 0, 11, 0, 3), (1, 4, 4, 3, 1),
    (1, 2, 1, 0, 11), (1, 2, 12, 4, 9), (0, 2, 0, 0, 0), (0, 3, 1, 0, 0), (0, 3, 12, 0, 0), (1, 2, 0, 2, 5),
    (0, 1, 9, 0, 0), (0, 1, 11, 0, 0), (0, 5, 4, 0, 0), (1, 1, 9, 1, 10), (1, 5, 4, 3, 1), (1, 1, 11, 0, 3),
    (1, 5, 15, 4, 13), (0, 0, 10, 0, 0), (0, 1, 5, 0, 0), (0, 4, 1, 0, 0), (1, 4, 4, 2, 0), (0, 0, 3, 0, 0),
    (0, 4, 13, 0, 0), (1, 0, 3, 3, 6), (1, 4, 13, 1, 12), (1, 0, 10, 4, 8), (1, 3, 1, 0, 11), (0, 1, 10, 0, 0),
    (0, 3, 0, 0, 0), (0, 5, 1, 0, 0), (1, 3, 0, 2, 5), (0, 2, 9, 0, 0), (0, 2, 11, 0, 0), (1, 2, 9, 1, 10),
    (1, 2, 11, 0, 3), (1, 3, 12, 4, 9), (0, 0, 6, 0, 0), (0, 2, 5, 0, 0), (0, 4, 12, 0, 0), (1, 5, 4, 2, 0),
    (0, 1, 3, 0, 0), (0, 5, 13, 0, 0), (1, 1, 3, 3, 6), (1, 5, 13, 1, 12), (1, 1, 10, 4, 8), (1, 4, 1, 0, 11),
    (0, 2, 10, 0, 0), (0, 4, 0, 0, 0), (1, 4, 0, 2, 5), (0, 0, 8, 0, 0), (0, 3, 11, 0, 0), (1, 0, 8, 1, 14),
    (1, 3, 11, 0, 3), (1, 4, 12, 4, 9), (0, 1, 6, 0, 0), (0, 3, 5, 0, 0), (0, 5, 12, 0, 0), (0, 2, 3, 0, 0),
    (0, 3, 9, 0, 0), (1, 2, 3, 3, 6), (1, 3, 9, 1, 10), (1, 2, 10, 4, 8), (1, 5, 1, 0, 11), (0, 0, 14, 0, 0),
    (0, 5, 0, 0, 0), (1, 0, 14, 3, 2), (1, 5, 0, 2, 5), (0, 1, 8, 0, 0), (0, 4, 11, 0, 0), (1, 1, 8, 1, 14),
    (1, 4, 11, 0, 3), (1, 5, 12, 4, 9), (0, 2, 6, 0, 0), (0, 3, 10, 0, 0), (0, 4, 5, 0, 0), (0, 3, 3, 0, 0),
    (0, 4, 9, 0, 0), (1, 3, 3, 3, 6), (1, 4, 9, 1, 10), (1, 3, 10, 4, 8), (0, 0, 2, 0, 0), (0, 1, 14, 0, 0),
    (0, 5, 5, 0, 0), (1, 1, 14, 3, 2), (0, 2, 8, 0, 0), (0, 5, 11, 0, 0), (1, 2, 8, 1, 14), (1, 5, 11, 0, 3),
    (1, 4, 15, 0, 7), (0, 3, 6, 0, 0), (0, 4, 10, 0, 0), (1, 4, 10, 4, 8), (0, 4, 3, 0, 0), (0, 5, 9, 0, 0),
    (1, 4, 3, 3, 6), (1, 5, 9, 1, 10), (1, 5, 15, 0, 7), (0, 1, 2, 0, 0), (0, 2, 14, 0, 0), (1, 2, 14, 3, 2),
    (0, 3, 8, 0, 0), (0, 5, 3, 0, 0), (1, 3, 8, 1, 14), (1, 5, 3, 3, 6), (0, 4, 6, 0, 0), (0, 5, 10, 0, 0),
    (1, 5, 10, 4, 8), (0, 4, 7, 0, 0), (0, 4, 8, 0, 0), (1, 4, 8, 1, 14), (0, 2, 2, 0, 0), (0, 3, 14, 0, 0),
    (1, 3, 14, 3, 2), (0, 5, 7, 0, 0), (0, 5, 8, 0, 0), (1, 5, 8, 1, 14), (0, 4, 14, 0, 0), (0, 5, 6, 0, 0),
    (1, 4, 14, 3, 2), (0, 3, 2, 0, 0), (0, 5, 14, 0, 0), (1, 5, 14, 3, 2), (0, 4, 2, 0, 0), (0, 5, 2, 0, 0),
)


NSLOT = len(OFFSETS)
CHUNKS = 1 + max(item[1] for item in PLAN)
OWN = OFFSETS.index((0, 0, 0))
STEPS = ((1, 0, 0), (3, 0, 0), (0, 1, 0), (0, 3, 0), (0, 0, 1), (0, 0, 7))
SIDES = (4, 4, 8)
MESH = pl.DeviceIdType.MESH
NI = 8
F32 = jnp.float32


def difference(first, second):
    return tuple((a - b) % side for a, b, side in zip(first, second, SIDES))


def weight_table():
    seen = set()
    table = np.zeros((NROW, 1, 128), np.float32)
    for row in range(NROW):
        for col in range(COLS):
            step = difference(OFFSETS[ROW0 + row], OFFSETS[col])
            back = difference((0, 0, 0), step)
            if min(step, back) in seen:
                continue
            seen.add(min(step, back))
            table[row, 0, col * 16 : col * 16 + 16] = 0.5 if step == back else 1.0
    assert len(seen) == 68
    return table


def kernel(
    x_ref, eps_ref, occ_ref, weight_ref, out_ref,
    raw, buf, acc, accr, epsbuf, epspart, pair_acc, square, vsrc, vrecv, csrc, crecv,
    plane, line,
    in_sem, part_send, part_recv, ring_send, ring_recv, eps_send, eps_recv,
    acc_send, acc_recv, v_send, v_recv, p_send, p_recv, l_send, l_recv,
):
    row = lax.axis_index("row")
    col = lax.axis_index("col")
    core = row % 2
    other = 1 - core
    cy = (row // 2) % 4
    cx = (col % 2) * 2 + row // 8
    cz = col // 2

    def device(step, which):
        x = (cx + step[0]) % 4
        y = (cy + step[1]) % 4
        z = (cz + step[2]) % 8
        return ((x % 2) * 8 + y * 2 + which, z * 2 + x // 2)

    partner = device((0, 0, 0), other)
    pending = []

    def send(src, dst, send_sem, recv_sem, target):
        copy = pltpu.make_async_remote_copy(
            src_ref=src, dst_ref=dst, send_sem=send_sem, recv_sem=recv_sem,
            device_id=target, device_id_type=MESH,
        )
        copy.start()
        pending.append(copy)
        return copy

    def arrived(ref, send_sem, recv_sem, target):
        pltpu.make_async_remote_copy(
            src_ref=ref, dst_ref=ref, send_sem=send_sem, recv_sem=recv_sem,
            device_id=target, device_id_type=MESH,
        ).wait_recv()

    half = x_ref.shape[1] // 2
    width = half // CHUNKS
    mine = pl.ds(pl.multiple_of(core * 64, 64), 64)
    theirs = pl.ds(pl.multiple_of(other * 64, 64), 64)
    local = pltpu.make_async_copy(
        x_ref.at[:, pl.ds(pl.multiple_of(core * half, 128), half)], raw.at[mine], in_sem
    )
    send(
        x_ref.at[:, pl.ds(pl.multiple_of(other * half, 128), half)], raw.at[mine],
        part_send.at[0], part_recv.at[0], partner,
    )
    local.start()
    send(eps_ref, epspart, part_send.at[1], part_recv.at[1], partner)

    lane = lax.broadcasted_iota(jnp.int32, (1, 128), 1)
    lane8 = lax.broadcasted_iota(jnp.int32, (8, 128), 1)
    sub8 = lax.broadcasted_iota(jnp.int32, (8, 128), 0)
    to = lax.broadcasted_iota(jnp.int32, (128, 128), 0)
    source = lax.broadcasted_iota(jnp.int32, (128, 128), 1)
    order = (source == ((to // 8) % 2) * 64 + (to % 8) * 8 + to // 16).astype(F32).astype(jnp.bfloat16)

    local.wait()
    arrived(raw.at[theirs], part_send.at[0], part_recv.at[0], partner)

    ready = set()

    def prepare(chunk):
        if chunk in ready:
            return
        ready.add(chunk)
        piece = raw[:, chunk * width : (chunk + 1) * width]
        buf[chunk, OWN] = jnp.dot(order, piece, preferred_element_type=F32).astype(jnp.bfloat16)

    def multiply(chunk, pair, first):
        count = min(2, NROW - 2 * pair)
        left = buf[chunk, ROW0 + 2 * pair : ROW0 + 2 * pair + count].reshape(count * 128, width)

        def one(block, carry):
            at = pl.multiple_of(block * 32, 32)
            right = jnp.concatenate(
                [
                    buf[chunk, 0:COLS, pl.ds(at + 16 * j, 16), :].reshape(COLS * 16, width)
                    for j in range(2)
                ],
                axis=0,
            )
            part = lax.dot_general(
                left, right, (((1,), (1,)), ((), ())), preferred_element_type=F32
            ).reshape(count, NI, 2, 8, 256)
            lanes = pl.ds(pl.multiple_of(block * 256, 256), 256)
            for k in range(count):
                for h in range(2):
                    where = (2 * pair + k, h, slice(None), slice(None), lanes)
                    if first:
                        acc[where] = part[k, :, h]
                    else:
                        acc[where] += part[k, :, h]
            return carry

        lax.fori_loop(0, 4, one, 0)

    def eps_exchange():
        arrived(epspart, part_send.at[1], part_recv.at[1], partner)
        epsbuf[OWN] = jnp.where((lane // 8) % 2 == core, eps_ref[...], epspart[...])
        for slot in range(NSLOT):
            if slot != OWN:
                send(
                    epsbuf.at[OWN], epsbuf.at[slot], eps_send.at[slot], eps_recv.at[slot],
                    device(OFFSETS[slot], core),
                )

    npair = (NROW + 1) // 2
    left_in = [NSLOT - 1] * CHUNKS
    queue = []
    sent = 0
    for kind, chunk, slot, step, target in PLAN:
        if kind == 0:
            arrived(
                buf.at[chunk, slot], ring_send.at[chunk, slot], ring_recv.at[chunk, slot], partner
            )
            left_in[chunk] -= 1
            if queue:
                multiply(*queue.pop(0))
            if left_in[chunk] == 0:
                queue += [(chunk, pair, chunk == FIRST) for pair in range(npair)]
        else:
            if slot == OWN:
                prepare(chunk)
            send(
                buf.at[chunk, slot], buf.at[chunk, target],
                ring_send.at[chunk, target], ring_recv.at[chunk, target],
                device(STEPS[step], core),
            )
            sent += 1
            if sent == 12:
                eps_exchange()

    def give(pair):
        for k in range(2 * pair, min(2 * pair + 2, NROW)):
            send(acc.at[k, other], accr.at[k], acc_send.at[k], acc_recv.at[k], partner)

    done = []
    while queue:
        chunk, pair, first = queue.pop(0)
        multiply(chunk, pair, first)
        if chunk == LAST:
            give(pair)
            done.append(pair)
    assert len(done) == npair

    for slot in range(NSLOT):
        if slot != OWN:
            arrived(epsbuf.at[slot], eps_send.at[slot], eps_recv.at[slot], partner)
    virt_col = jnp.zeros((1, 128), F32)
    for slot in range(COLS):
        virt_col = jnp.where(lane // 16 == slot, epsbuf[slot], virt_col)
    virt_col = jnp.broadcast_to(virt_col, (8, 128))
    pair_acc[...] = jnp.zeros_like(pair_acc)
    square[...] = jnp.zeros_like(square)

    def energy(k, col_sum):
        arrived(accr.at[k], acc_send.at[k], acc_recv.at[k], partner)
        spread = jnp.broadcast_to(epsbuf[ROW0 + k], (8, 128))
        virt_row = jnp.sum(
            jnp.where(lane8 == 8 * core + sub8, spread, 0.0), axis=1, keepdims=True
        )
        virt = virt_row + virt_col
        weight = jnp.broadcast_to(weight_ref[k], (8, 128))
        total = jnp.zeros((8, 128), F32)
        count = 0
        for i in range(NI):
            for j in range(i, NI):
                here = slice(128 * j, 128 * j + 128)
                there = slice(128 * i, 128 * i + 128)
                scale = weight / ((occ_ref[i] + occ_ref[j]) - virt)
                t = acc[k, core, i, :, here] + accr[k, i, :, here]
                if i == j:
                    term = t * t * scale
                    pair_acc[count] += 2.0 * term
                else:
                    s = acc[k, core, j, :, there] + accr[k, j, :, there]
                    term = (t * (2.0 * t - s) + s * (2.0 * s - t)) * scale
                    pair_acc[count] += term
                total += term
                count += 1
        square[pl.ds(pl.multiple_of(k * 8, 8), 8), :] = total
        return col_sum + total

    col_sum = lax.fori_loop(0, NROW, energy, jnp.zeros((8, 128), F32))
    vsrc[:, 0:128] = jnp.sum(square[...].T, axis=0, keepdims=True)
    vsrc[:, 128:256] = jnp.sum(col_sum, axis=0, keepdims=True)

    here = cx * 4 + cy
    count = 0
    square[...] = jnp.zeros_like(square)
    for i in range(NI):
        for j in range(i, NI):
            total = jnp.sum(pair_acc[count], axis=0, keepdims=True)
            square[i * 8 + j : i * 8 + j + 1, :] = total
            square[j * 8 + i : j * 8 + i + 1, :] = total
            count += 1
    plane[here] = jnp.sum(square[...].T, axis=0, keepdims=True)
    for m in range(1, 16):
        send(
            plane.at[here], plane.at[here], p_send.at[m], p_recv.at[m],
            device((m // 4, m % 4, 0), core),
        )

    used = [s for s in range(NSLOT) if s != OWN and (s < COLS or ROW0 <= s < ROW0 + NROW)]
    for slot in used:
        step = difference((0, 0, 0), OFFSETS[slot])
        send(vsrc, vrecv.at[slot], v_send.at[slot], v_recv.at[slot], device(step, core))
    row_total = jnp.zeros((1, 128), F32)
    col_total = jnp.zeros((1, 128), F32)
    for slot in used + [OWN]:
        if slot == OWN:
            message = vsrc[...]
        else:
            arrived(vrecv.at[slot], v_send.at[slot], v_recv.at[slot], partner)
            message = vrecv[slot]
        if ROW0 <= slot < ROW0 + NROW:
            row_total += jnp.where(lane // 8 == slot - ROW0, message[:, 0:128], 0.0)
        if slot < COLS:
            col_total += jnp.where(lane // 16 == slot, message[:, 128:256], 0.0)
    csrc[...] = col_total
    send(csrc, crecv, part_send.at[2], part_recv.at[2], partner)

    def gathered(ref, index, send_sem, recv_sem):
        arrived(ref.at[index], send_sem, recv_sem, partner)

    for m in range(1, 16):
        x = (cx + 4 - m // 4) % 4
        y = (cy + 4 - m % 4) % 4
        gathered(plane, x * 4 + y, p_send.at[m], p_recv.at[m])
    now = cz * 2 + core
    line[now] = jnp.sum(plane[...], axis=0)
    for m in range(1, 16):
        which = core if m % 2 == 0 else other
        send(
            line.at[now], line.at[now], l_send.at[m], l_recv.at[m],
            device((0, 0, m // 2), which),
        )
    arrived(crecv, part_send.at[2], part_recv.at[2], partner)
    virt = row_total + jnp.where((lane // 8) % 2 == core, col_total + crecv[...], 0.0)

    def fold(value):
        for shift in (64, 32, 16, 8):
            value = value + pltpu.roll(value, shift, 1)
        return value

    out_ref[8:16, :] = fold(jnp.broadcast_to(virt, (8, 128)))
    for m in range(1, 16):
        z = (cz + 8 - m // 2) % 8
        which = core if m % 2 == 0 else other
        gathered(line, z * 2 + which, l_send.at[m], l_recv.at[m])
    total = jnp.broadcast_to(jnp.sum(line[...], axis=0), (8, 128))
    out_ref[0:8, :] = fold(jnp.where(lane8 // 8 == sub8, total, 0.0))
    for copy in pending:
        copy.wait_send()


def on_device(orbital_factors, occ_energy, virt_energy):
    naux = orbital_factors.shape[2]
    width = naux // 2 // CHUNKS
    eps = jnp.tile(virt_energy.astype(F32), 16).reshape(1, 128)
    vmem = pl.BlockSpec(memory_space=pltpu.VMEM)
    dma = pltpu.SemaphoreType.DMA
    out = pl.pallas_call(
        kernel,
        out_shape=jax.ShapeDtypeStruct((16, 128), F32),
        in_specs=[pl.BlockSpec(memory_space=pl.ANY), vmem, pl.BlockSpec(memory_space=pltpu.SMEM), vmem],
        out_specs=vmem,
        scratch_shapes=[
            pltpu.VMEM((128, naux // 2), jnp.bfloat16),
            pltpu.VMEM((CHUNKS, NSLOT, 128, width), jnp.bfloat16),
            pltpu.VMEM((NROW, 2, NI, 8, 1024), F32),
            pltpu.VMEM((NROW, NI, 8, 1024), F32),
            pltpu.VMEM((NSLOT, 1, 128), F32),
            pltpu.VMEM((1, 128), F32),
            pltpu.VMEM((36, 8, 128), F32),
            pltpu.VMEM((128, 128), F32),
            pltpu.VMEM((1, 256), F32),
            pltpu.VMEM((NSLOT, 1, 256), F32),
            pltpu.VMEM((1, 128), F32),
            pltpu.VMEM((1, 128), F32),
            pltpu.VMEM((16, 1, 128), F32),
            pltpu.VMEM((16, 1, 128), F32),
            dma(()),
            dma((3,)), dma((3,)),
            dma((CHUNKS, NSLOT)), dma((CHUNKS, NSLOT)),
            dma((NSLOT,)), dma((NSLOT,)),
            dma((NROW,)), dma((NROW,)),
            dma((NSLOT,)), dma((NSLOT,)),
            dma((16,)), dma((16,)),
            dma((16,)), dma((16,)),
        ],
        compiler_params=pltpu.CompilerParams(
            has_side_effects=True, vmem_limit_bytes=60 * 2**20
        ),
    )(
        orbital_factors.reshape(-1, naux), eps, occ_energy.astype(F32), jnp.asarray(weight_table()),
    )
    return out[0:8, 0:8], out[8, 0:8]


def solution(mesh):
    return jax.shard_map(
        on_device,
        mesh=mesh,
        in_specs=(P(("row", "col"), None, None), P(), P(("row", "col"))),
        out_specs=(P(), P(("row", "col"))),
        check_vma=False,
    )
```

```python
import functools

import jax
import jax.numpy as jnp
import numpy as np
from jax import lax
from jax.experimental import pallas as pl
from jax.experimental.pallas import tpu as pltpu
from jax.sharding import PartitionSpec as P

OFFSETS = (
    (0, 1, 7),
    (0, 3, 7),
    (1, 3, 3),
    (2, 3, 7),
    (0, 0, 7),
    (0, 2, 7),
    (2, 2, 7),
    (1, 0, 0),
    (2, 0, 3),
    (3, 0, 2),
    (2, 0, 2),
    (1, 3, 7),
    (3, 0, 1),
    (0, 0, 1),
    (1, 0, 3),
    (0, 0, 0),
)
COLS = 8
ROW0 = 5
NROW = 11
FIRST = 0
LAST = 5
PLAN = (
    (1, 0, 15, 0, 7), (1, 0, 15, 4, 13), (1, 0, 15, 5, 4), (1, 1, 15, 0, 7), (1, 1, 15, 4, 13), (1, 1, 15, 5, 4),
    (1, 2, 15, 0, 7), (1, 2, 15, 4, 13), (1, 2, 15, 5, 4), (0, 0, 4, 0, 0), (0, 0, 7, 0, 0), (0, 0, 13, 0, 0),
    (1, 0, 4, 2, 0), (1, 0, 4, 3, 1), (1, 0, 13, 1, 12), (1, 3, 15, 0, 7), (1, 3, 15, 4, 13), (1, 3, 15, 5, 4),
    (0, 1, 4, 0, 0), (0, 1, 7, 0, 0), (0, 1, 13, 0, 0), (1, 1, 4, 2, 0), (1, 1, 4, 3, 1), (1, 1, 13, 1, 12),
    (1, 4, 15, 5, 4), (0, 0, 0, 0, 0), (0, 0, 1, 0, 0), (0, 0, 12, 0, 0), (1, 0, 0, 2, 5), (1, 0, 1, 0, 11),
    (1, 0, 12, 4, 9), (0, 2, 4, 0, 0), (0, 2, 7, 0, 0), (0, 2, 13, 0, 0), (1, 2, 4, 2, 0), (1, 2, 4, 3, 1),
    (1, 2, 13, 1, 12), (1, 5, 15, 5, 4), (0, 1, 0, 0, 0), (0, 1, 1, 0, 0), (0, 1, 12, 0, 0), (1, 1, 1, 0, 11),
    (1, 1, 12, 4, 9), (1, 1, 0, 2, 5), (0, 3, 4, 0, 0), (0, 3, 7, 0, 0), (0, 3, 13, 0, 0), (1, 3, 4, 3, 1),
    (1, 3, 13, 1, 12), (1, 4, 15, 4, 13), (0, 0, 5, 0, 0), (0, 2, 1, 0, 0), (0, 2, 12, 0, 0), (1, 3, 4, 2, 0),
    (0, 0, 9, 0, 0), (0, 0, 11, 0, 0), (0, 4, 4, 0, 0), (1, 0, 9, 1, 10), (1, 0, 11, 0, 3), (1, 4, 4, 3, 1),
    (1, 2, 1, 0, 11), (1, 2, 12, 4, 9), (0, 2, 0, 0, 0), (0, 3, 1, 0, 0), (0, 3, 12, 0, 0), (1, 2, 0, 2, 5),
    (0, 1, 9, 0, 0), (0, 1, 11, 0, 0), (0, 5, 4, 0, 0), (1, 1, 9, 1, 10), (1, 5, 4, 3, 1), (1, 1, 11, 0, 3),
    (1, 5, 15, 4, 13), (0, 0, 10, 0, 0), (0, 1, 5, 0, 0), (0, 4, 1, 0, 0), (1, 4, 4, 2, 0), (0, 0, 3, 0, 0),
    (0, 4, 13, 0, 0), (1, 0, 3, 3, 6), (1, 4, 13, 1, 12), (1, 0, 10, 4, 8), (1, 3, 1, 0, 11), (0, 1, 10, 0, 0),
    (0, 3, 0, 0, 0), (0, 5, 1, 0, 0), (1, 3, 0, 2, 5), (0, 2, 9, 0, 0), (0, 2, 11, 0, 0), (1, 2, 9, 1, 10),
    (1, 2, 11, 0, 3), (1, 3, 12, 4, 9), (0, 0, 6, 0, 0), (0, 2, 5, 0, 0), (0, 4, 12, 0, 0), (1, 5, 4, 2, 0),
    (0, 1, 3, 0, 0), (0, 5, 13, 0, 0), (1, 1, 3, 3, 6), (1, 5, 13, 1, 12), (1, 1, 10, 4, 8), (1, 4, 1, 0, 11),
    (0, 2, 10, 0, 0), (0, 4, 0, 0, 0), (1, 4, 0, 2, 5), (0, 0, 8, 0, 0), (0, 3, 11, 0, 0), (1, 0, 8, 1, 14),
    (1, 3, 11, 0, 3), (1, 4, 12, 4, 9), (0, 1, 6, 0, 0), (0, 3, 5, 0, 0), (0, 5, 12, 0, 0), (0, 2, 3, 0, 0),
    (0, 3, 9, 0, 0), (1, 2, 3, 3, 6), (1, 3, 9, 1, 10), (1, 2, 10, 4, 8), (1, 5, 1, 0, 11), (0, 0, 14, 0, 0),
    (0, 5, 0, 0, 0), (1, 0, 14, 3, 2), (1, 5, 0, 2, 5), (0, 1, 8, 0, 0), (0, 4, 11, 0, 0), (1, 1, 8, 1, 14),
    (1, 4, 11, 0, 3), (1, 5, 12, 4, 9), (0, 2, 6, 0, 0), (0, 3, 10, 0, 0), (0, 4, 5, 0, 0), (0, 3, 3, 0, 0),
    (0, 4, 9, 0, 0), (1, 3, 3, 3, 6), (1, 4, 9, 1, 10), (1, 3, 10, 4, 8), (0, 0, 2, 0, 0), (0, 1, 14, 0, 0),
    (0, 5, 5, 0, 0), (1, 1, 14, 3, 2), (0, 2, 8, 0, 0), (0, 5, 11, 0, 0), (1, 2, 8, 1, 14), (1, 5, 11, 0, 3),
    (1, 4, 15, 0, 7), (0, 3, 6, 0, 0), (0, 4, 10, 0, 0), (1, 4, 10, 4, 8), (0, 4, 3, 0, 0), (0, 5, 9, 0, 0),
    (1, 4, 3, 3, 6), (1, 5, 9, 1, 10), (1, 5, 15, 0, 7), (0, 1, 2, 0, 0), (0, 2, 14, 0, 0), (1, 2, 14, 3, 2),
    (0, 3, 8, 0, 0), (0, 5, 3, 0, 0), (1, 3, 8, 1, 14), (1, 5, 3, 3, 6), (0, 4, 6, 0, 0), (0, 5, 10, 0, 0),
    (1, 5, 10, 4, 8), (0, 4, 7, 0, 0), (0, 4, 8, 0, 0), (1, 4, 8, 1, 14), (0, 2, 2, 0, 0), (0, 3, 14, 0, 0),
    (1, 3, 14, 3, 2), (0, 5, 7, 0, 0), (0, 5, 8, 0, 0), (1, 5, 8, 1, 14), (0, 4, 14, 0, 0), (0, 5, 6, 0, 0),
    (1, 4, 14, 3, 2), (0, 3, 2, 0, 0), (0, 5, 14, 0, 0), (1, 5, 14, 3, 2), (0, 4, 2, 0, 0), (0, 5, 2, 0, 0),
)


NSLOT = len(OFFSETS)
CHUNKS = 1 + max(item[1] for item in PLAN)
OWN = OFFSETS.index((0, 0, 0))
STEPS = ((1, 0, 0), (3, 0, 0), (0, 1, 0), (0, 3, 0), (0, 0, 1), (0, 0, 7))
SIDES = (4, 4, 8)
MESH = pl.DeviceIdType.MESH
NI = 8
GROUP = 4
F32 = jnp.float32


def difference(first, second):
    return tuple((a - b) % side for a, b, side in zip(first, second, SIDES))


def weight_table():
    seen = set()
    table = np.zeros((NROW, 1, 128), np.float32)
    for row in range(NROW):
        for col in range(COLS):
            step = difference(OFFSETS[ROW0 + row], OFFSETS[col])
            back = difference((0, 0, 0), step)
            if min(step, back) in seen:
                continue
            seen.add(min(step, back))
            table[row, 0, col * 16 : col * 16 + 16] = 0.5 if step == back else 1.0
    assert len(seen) == 68
    return table


def kernel(
    x_ref, eps_ref, occ_ref, weight_ref, out_ref,
    raw, buf, acc, accr, epsbuf, epspart, pair_acc, square, vsrc, vrecv, csrc, crecv,
    plane, line,
    in_sem, part_send, part_recv, ring_send, ring_recv, eps_send, eps_recv,
    acc_send, acc_recv, v_send, v_recv, p_send, p_recv, l_send, l_recv,
):
    row = lax.axis_index("row")
    col = lax.axis_index("col")
    core = row % 2
    other = 1 - core
    cy = (row // 2) % 4
    cx = (col % 2) * 2 + row // 8
    cz = col // 2

    def device(step, which):
        x = (cx + step[0]) % 4
        y = (cy + step[1]) % 4
        z = (cz + step[2]) % 8
        return ((x % 2) * 8 + y * 2 + which, z * 2 + x // 2)

    partner = device((0, 0, 0), other)
    pending = []

    def send(src, dst, send_sem, recv_sem, target):
        copy = pltpu.make_async_remote_copy(
            src_ref=src, dst_ref=dst, send_sem=send_sem, recv_sem=recv_sem,
            device_id=target, device_id_type=MESH,
        )
        copy.start()
        pending.append(copy)
        return copy

    def arrived(ref, send_sem, recv_sem, target):
        pltpu.make_async_remote_copy(
            src_ref=ref, dst_ref=ref, send_sem=send_sem, recv_sem=recv_sem,
            device_id=target, device_id_type=MESH,
        ).wait_recv()

    peers = {(0, 0, 0, 1)}
    for offset in OFFSETS:
        peers |= {offset + (0,), difference((0, 0, 0), offset) + (0,)}
    peers |= {step + (0,) for step in STEPS}
    peers |= {(m // 4, m % 4, 0, 0) for m in range(16)}
    peers |= {(0, 0, m // 2, m % 2) for m in range(16)}
    peers -= {(0, 0, 0, 0)}
    barrier = pltpu.get_barrier_semaphore()
    for peer in sorted(peers):
        pl.semaphore_signal(
            barrier, inc=1, device_id=device(peer[:3], other if peer[3] else core),
            device_id_type=MESH,
        )
    pl.semaphore_wait(barrier, len(peers))

    half = x_ref.shape[1] // 2
    width = half // CHUNKS
    mine = pl.ds(pl.multiple_of(core * 64, 64), 64)
    theirs = pl.ds(pl.multiple_of(other * 64, 64), 64)
    local = pltpu.make_async_copy(
        x_ref.at[:, pl.ds(pl.multiple_of(core * half, 128), half)], raw.at[mine], in_sem
    )
    send(
        x_ref.at[:, pl.ds(pl.multiple_of(other * half, 128), half)], raw.at[mine],
        part_send.at[0], part_recv.at[0], partner,
    )
    local.start()
    send(eps_ref, epspart, part_send.at[1], part_recv.at[1], partner)

    lane = lax.broadcasted_iota(jnp.int32, (1, 128), 1)
    lane8 = lax.broadcasted_iota(jnp.int32, (8, 128), 1)
    sub8 = lax.broadcasted_iota(jnp.int32, (8, 128), 0)
    to = lax.broadcasted_iota(jnp.int32, (128, 128), 0)
    source = lax.broadcasted_iota(jnp.int32, (128, 128), 1)
    order = (source == ((to // 8) % 2) * 64 + (to % 8) * 8 + to // 16).astype(F32).astype(jnp.bfloat16)

    local.wait()
    arrived(raw.at[theirs], part_send.at[0], part_recv.at[0], partner)

    ready = set()

    def prepare(chunk):
        if chunk in ready:
            return
        ready.add(chunk)
        piece = raw[:, chunk * width : (chunk + 1) * width]
        buf[chunk, OWN] = jnp.dot(order, piece, preferred_element_type=F32).astype(jnp.bfloat16)

    def multiply(chunk, block):
        right = jnp.concatenate(
            [
                buf[chunk, 0:COLS, 16 * j : 16 * j + 16, :].reshape(COLS * 16, width)
                for j in (2 * block, 2 * block + 1)
            ],
            axis=0,
        )
        lanes = slice(256 * block, 256 * block + 256)
        for k in range(0, NROW, GROUP):
            count = min(GROUP, NROW - k)
            left = buf[chunk, ROW0 + k : ROW0 + k + count].reshape(count * 128, width)
            part = lax.dot_general(
                left, right, (((1,), (1,)), ((), ())), preferred_element_type=F32
            ).reshape(count, NI, 2, 8, 256)
            for h in range(2):
                if chunk == FIRST:
                    acc[k : k + count, h, :, :, lanes] = part[:, :, h]
                else:
                    acc[k : k + count, h, :, :, lanes] += part[:, :, h]

    def eps_exchange():
        arrived(epspart, part_send.at[1], part_recv.at[1], partner)
        epsbuf[OWN] = jnp.where((lane // 8) % 2 == core, eps_ref[...], epspart[...])
        for slot in range(NSLOT):
            if slot != OWN:
                send(
                    epsbuf.at[OWN], epsbuf.at[slot], eps_send.at[slot], eps_recv.at[slot],
                    device(OFFSETS[slot], core),
                )

    left_in = [NSLOT - 1] * CHUNKS
    queue = []
    sent = 0
    for kind, chunk, slot, step, target in PLAN:
        if kind == 0:
            arrived(
                buf.at[chunk, slot], ring_send.at[chunk, slot], ring_recv.at[chunk, slot], partner
            )
            left_in[chunk] -= 1
            if queue:
                multiply(*queue.pop(0))
            if left_in[chunk] == 0:
                queue += [(chunk, block) for block in range(4)]
        else:
            if slot == OWN:
                prepare(chunk)
            send(
                buf.at[chunk, slot], buf.at[chunk, target],
                ring_send.at[chunk, target], ring_recv.at[chunk, target],
                device(STEPS[step], core),
            )
            sent += 1
            if sent == 12:
                eps_exchange()

    for chunk, block in queue:
        multiply(chunk, block)
        if chunk == LAST:
            lanes = slice(256 * block, 256 * block + 256)
            send(
                acc.at[:, other, :, :, lanes], accr.at[:, :, :, lanes],
                acc_send.at[block], acc_recv.at[block], partner,
            )

    for slot in range(NSLOT):
        if slot != OWN:
            arrived(epsbuf.at[slot], eps_send.at[slot], eps_recv.at[slot], partner)
    virt_col = jnp.zeros((1, 128), F32)
    for slot in range(COLS):
        virt_col = jnp.where(lane // 16 == slot, epsbuf[slot], virt_col)
    virt_col = jnp.broadcast_to(virt_col, (8, 128))
    pair_acc[...] = jnp.zeros_like(pair_acc)
    square[...] = jnp.zeros_like(square)

    for block in range(4):
        lanes = slice(256 * block, 256 * block + 256)
        arrived(accr.at[:, :, :, lanes], acc_send.at[block], acc_recv.at[block], partner)

    def energy(k, col_sum):
        spread = jnp.broadcast_to(epsbuf[ROW0 + k], (8, 128))
        virt_row = jnp.sum(
            jnp.where(lane8 == 8 * core + sub8, spread, 0.0), axis=1, keepdims=True
        )
        virt = virt_row + virt_col
        weight = jnp.broadcast_to(weight_ref[k], (8, 128))
        total = jnp.zeros((8, 128), F32)
        count = 0
        for i in range(NI):
            for j in range(i, NI):
                here = slice(128 * j, 128 * j + 128)
                there = slice(128 * i, 128 * i + 128)
                scale = weight / ((occ_ref[i] + occ_ref[j]) - virt)
                t = acc[k, core, i, :, here] + accr[k, i, :, here]
                if i == j:
                    term = t * t * scale
                    pair_acc[count] += 2.0 * term
                else:
                    s = acc[k, core, j, :, there] + accr[k, j, :, there]
                    term = (t * (2.0 * t - s) + s * (2.0 * s - t)) * scale
                    pair_acc[count] += term
                total += term
                count += 1
        square[pl.ds(pl.multiple_of(k * 8, 8), 8), :] = total
        return col_sum + total

    col_sum = lax.fori_loop(0, NROW, energy, jnp.zeros((8, 128), F32))
    vsrc[:, 0:128] = jnp.sum(square[...].T, axis=0, keepdims=True)
    vsrc[:, 128:256] = jnp.sum(col_sum, axis=0, keepdims=True)

    here = cx * 4 + cy
    count = 0
    square[...] = jnp.zeros_like(square)
    for i in range(NI):
        for j in range(i, NI):
            total = jnp.sum(pair_acc[count], axis=0, keepdims=True)
            square[i * 8 + j : i * 8 + j + 1, :] = total
            square[j * 8 + i : j * 8 + i + 1, :] = total
            count += 1
    plane[here] = jnp.sum(square[...].T, axis=0, keepdims=True)
    for m in range(1, 16):
        send(
            plane.at[here], plane.at[here], p_send.at[m], p_recv.at[m],
            device((m // 4, m % 4, 0), core),
        )

    used = [s for s in range(NSLOT) if s != OWN and (s < COLS or ROW0 <= s < ROW0 + NROW)]
    for slot in used:
        step = difference((0, 0, 0), OFFSETS[slot])
        send(vsrc, vrecv.at[slot], v_send.at[slot], v_recv.at[slot], device(step, core))
    row_total = jnp.zeros((1, 128), F32)
    col_total = jnp.zeros((1, 128), F32)
    for slot in used + [OWN]:
        if slot == OWN:
            message = vsrc[...]
        else:
            arrived(vrecv.at[slot], v_send.at[slot], v_recv.at[slot], partner)
            message = vrecv[slot]
        if ROW0 <= slot < ROW0 + NROW:
            row_total += jnp.where(lane // 8 == slot - ROW0, message[:, 0:128], 0.0)
        if slot < COLS:
            col_total += jnp.where(lane // 16 == slot, message[:, 128:256], 0.0)
    csrc[...] = col_total
    send(csrc, crecv, part_send.at[2], part_recv.at[2], partner)

    def gathered(ref, index, send_sem, recv_sem):
        arrived(ref.at[index], send_sem, recv_sem, partner)

    for m in range(1, 16):
        x = (cx + 4 - m // 4) % 4
        y = (cy + 4 - m % 4) % 4
        gathered(plane, x * 4 + y, p_send.at[m], p_recv.at[m])
    now = cz * 2 + core
    line[now] = jnp.sum(plane[...], axis=0)
    for m in range(1, 16):
        which = core if m % 2 == 0 else other
        send(
            line.at[now], line.at[now], l_send.at[m], l_recv.at[m],
            device((0, 0, m // 2), which),
        )
    arrived(crecv, part_send.at[2], part_recv.at[2], partner)
    virt = row_total + jnp.where((lane // 8) % 2 == core, col_total + crecv[...], 0.0)

    def fold(value):
        for shift in (64, 32, 16, 8):
            value = value + pltpu.roll(value, shift, 1)
        return value

    out_ref[8:16, :] = fold(jnp.broadcast_to(virt, (8, 128)))
    for m in range(1, 16):
        z = (cz + 8 - m // 2) % 8
        which = core if m % 2 == 0 else other
        gathered(line, z * 2 + which, l_send.at[m], l_recv.at[m])
    total = jnp.broadcast_to(jnp.sum(line[...], axis=0), (8, 128))
    out_ref[0:8, :] = fold(jnp.where(lane8 // 8 == sub8, total, 0.0))
    for copy in pending:
        copy.wait_send()


def on_device(orbital_factors, occ_energy, virt_energy):
    naux = orbital_factors.shape[2]
    width = naux // 2 // CHUNKS
    eps = jnp.tile(virt_energy.astype(F32), 16).reshape(1, 128)
    vmem = pl.BlockSpec(memory_space=pltpu.VMEM)
    dma = pltpu.SemaphoreType.DMA
    out = pl.pallas_call(
        kernel,
        out_shape=jax.ShapeDtypeStruct((16, 128), F32),
        in_specs=[pl.BlockSpec(memory_space=pl.ANY), vmem, pl.BlockSpec(memory_space=pltpu.SMEM), vmem],
        out_specs=vmem,
        scratch_shapes=[
            pltpu.VMEM((128, naux // 2), jnp.bfloat16),
            pltpu.VMEM((CHUNKS, NSLOT, 128, width), jnp.bfloat16),
            pltpu.VMEM((NROW, 2, NI, 8, 1024), F32),
            pltpu.VMEM((NROW, NI, 8, 1024), F32),
            pltpu.VMEM((NSLOT, 1, 128), F32),
            pltpu.VMEM((1, 128), F32),
            pltpu.VMEM((36, 8, 128), F32),
            pltpu.VMEM((128, 128), F32),
            pltpu.VMEM((1, 256), F32),
            pltpu.VMEM((NSLOT, 1, 256), F32),
            pltpu.VMEM((1, 128), F32),
            pltpu.VMEM((1, 128), F32),
            pltpu.VMEM((16, 1, 128), F32),
            pltpu.VMEM((16, 1, 128), F32),
            dma(()),
            dma((3,)), dma((3,)),
            dma((CHUNKS, NSLOT)), dma((CHUNKS, NSLOT)),
            dma((NSLOT,)), dma((NSLOT,)),
            dma((4,)), dma((4,)),
            dma((NSLOT,)), dma((NSLOT,)),
            dma((16,)), dma((16,)),
            dma((16,)), dma((16,)),
        ],
        compiler_params=pltpu.CompilerParams(
            collective_id=0, has_side_effects=True, vmem_limit_bytes=60 * 2**20
        ),
    )(
        orbital_factors.reshape(-1, naux), eps, occ_energy.astype(F32), jnp.asarray(weight_table()),
    )
    return out[0:8, 0:8], out[8, 0:8]


def solution(mesh):
    return jax.shard_map(
        on_device,
        mesh=mesh,
        in_specs=(P(("row", "col"), None, None), P(), P(("row", "col"))),
        out_specs=(P(), P(("row", "col"))),
        check_vma=False,
    )
```

```python
import functools

import jax
import jax.numpy as jnp
import numpy as np
from jax import lax
from jax.experimental import pallas as pl
from jax.experimental.pallas import tpu as pltpu
from jax.sharding import PartitionSpec as P

OFFSETS = (
    (1, 0, 3),
    (1, 0, 7),
    (2, 2, 7),
    (0, 3, 7),
    (3, 3, 7),
    (2, 0, 7),
    (0, 0, 3),
    (1, 2, 7),
    (0, 0, 7),
    (0, 0, 2),
    (0, 1, 1),
    (0, 0, 1),
    (0, 1, 0),
    (0, 1, 2),
    (0, 0, 0),
    (2, 3, 7),
)
COLS = 8
ROW0 = 6
NROW = 10
FIRST = 0
LAST = 5
PLAN = (
    (1, 0, 14, 2, 12), (1, 0, 14, 4, 11), (1, 0, 14, 5, 8), (1, 1, 14, 2, 12), (1, 1, 14, 4, 11), (1, 1, 14, 5, 8),
    (0, 0, 8, 0, 0), (0, 0, 11, 0, 0), (0, 0, 12, 0, 0), (1, 0, 8, 0, 1), (1, 0, 8, 3, 3), (1, 0, 11, 2, 10),
    (1, 0, 11, 4, 9), (1, 2, 14, 5, 8), (0, 1, 8, 0, 0), (0, 1, 11, 0, 0), (0, 1, 12, 0, 0), (1, 1, 8, 0, 1),
    (1, 1, 8, 3, 3), (1, 1, 11, 2, 10), (1, 2, 14, 4, 11), (1, 3, 14, 5, 8), (0, 0, 1, 0, 0), (0, 0, 3, 0, 0),
    (1, 0, 3, 1, 4), (0, 0, 9, 0, 0), (0, 0, 10, 0, 0), (0, 2, 8, 0, 0), (1, 0, 1, 0, 5), (1, 2, 8, 3, 3),
    (1, 0, 9, 2, 13), (1, 1, 11, 4, 9), (1, 4, 14, 5, 8), (0, 1, 1, 0, 0), (0, 1, 3, 0, 0), (1, 1, 3, 1, 4),
    (0, 1, 10, 0, 0), (0, 2, 11, 0, 0), (0, 3, 8, 0, 0), (1, 1, 1, 0, 5), (1, 3, 8, 3, 3), (1, 0, 9, 4, 6),
    (1, 2, 14, 2, 12), (1, 5, 14, 5, 8), (0, 0, 4, 0, 0), (0, 0, 5, 0, 0), (0, 2, 3, 0, 0), (1, 0, 4, 1, 15),
    (0, 0, 13, 0, 0), (0, 1, 9, 0, 0), (0, 4, 8, 0, 0), (1, 3, 8, 0, 1), (1, 4, 8, 3, 3), (1, 1, 9, 2, 13),
    (1, 3, 14, 4, 11), (0, 1, 4, 0, 0), (0, 1, 5, 0, 0), (0, 3, 3, 0, 0), (1, 2, 3, 1, 4), (0, 0, 6, 0, 0),
    (0, 2, 12, 0, 0), (0, 5, 8, 0, 0), (1, 1, 5, 3, 15), (1, 4, 8, 0, 1), (1, 2, 11, 2, 10), (1, 2, 11, 4, 9),
    (0, 0, 15, 0, 0), (0, 3, 1, 0, 0), (0, 4, 3, 0, 0), (1, 3, 3, 1, 4), (0, 1, 13, 0, 0), (0, 3, 11, 0, 0),
    (1, 0, 15, 3, 2), (1, 3, 1, 0, 5), (1, 1, 9, 4, 6), (1, 3, 11, 2, 10), (0, 2, 4, 0, 0), (0, 1, 15, 0, 0),
    (0, 4, 1, 0, 0), (1, 2, 4, 1, 15), (0, 2, 9, 0, 0), (0, 2, 10, 0, 0), (1, 0, 6, 0, 0), (1, 1, 15, 3, 2),
    (1, 2, 9, 2, 13), (1, 4, 14, 4, 11), (0, 3, 4, 0, 0), (0, 0, 2, 0, 0), (0, 3, 5, 0, 0), (1, 0, 2, 1, 7),
    (0, 1, 6, 0, 0), (0, 3, 10, 0, 0), (1, 3, 10, 5, 12), (1, 4, 1, 0, 5), (1, 5, 8, 3, 3), (1, 3, 11, 4, 9),
    (1, 4, 14, 2, 12), (0, 2, 15, 0, 0), (0, 0, 0, 0, 0), (0, 1, 2, 0, 0), (1, 1, 2, 1, 7), (0, 2, 13, 0, 0),
    (0, 4, 11, 0, 0), (1, 2, 8, 0, 1), (1, 3, 5, 3, 15), (1, 2, 9, 4, 6), (1, 4, 11, 2, 10), (0, 0, 7, 0, 0),
    (0, 3, 12, 0, 0), (0, 4, 5, 0, 0), (0, 5, 3, 0, 0), (1, 5, 3, 1, 4), (0, 3, 9, 0, 0), (0, 4, 12, 0, 0),
    (1, 1, 6, 0, 0), (1, 2, 15, 3, 2), (1, 3, 9, 2, 13), (1, 5, 14, 4, 11), (0, 1, 7, 0, 0), (0, 2, 1, 0, 0),
    (0, 3, 15, 0, 0), (1, 4, 3, 1, 4), (0, 2, 6, 0, 0), (0, 4, 10, 0, 0), (1, 2, 1, 0, 5), (1, 4, 5, 3, 15),
    (1, 4, 11, 4, 9), (1, 5, 14, 2, 12), (0, 5, 4, 0, 0), (0, 1, 0, 0, 0), (0, 2, 2, 0, 0), (1, 2, 2, 1, 7),
    (0, 3, 13, 0, 0), (0, 5, 11, 0, 0), (1, 2, 6, 0, 0), (1, 3, 15, 3, 2), (1, 3, 9, 4, 6), (1, 5, 11, 2, 10),
    (0, 4, 4, 0, 0), (0, 2, 5, 0, 0), (0, 4, 15, 0, 0), (1, 5, 4, 1, 15), (0, 4, 9, 0, 0), (0, 5, 12, 0, 0),
    (1, 4, 15, 3, 2), (1, 5, 8, 0, 1), (1, 4, 9, 2, 13), (1, 5, 11, 4, 9), (0, 2, 7, 0, 0), (0, 2, 0, 0, 0),
    (0, 3, 2, 0, 0), (1, 3, 2, 1, 7), (0, 3, 6, 0, 0), (0, 5, 10, 0, 0), (1, 3, 6, 0, 0), (1, 4, 9, 4, 6),
    (0, 5, 15, 0, 0), (1, 5, 15, 3, 2), (0, 4, 2, 0, 0), (0, 5, 1, 0, 0), (1, 4, 2, 1, 7), (0, 4, 13, 0, 0),
    (0, 5, 9, 0, 0), (1, 5, 1, 0, 5), (1, 5, 9, 2, 13), (1, 5, 9, 4, 6), (0, 3, 7, 0, 0), (0, 3, 0, 0, 0),
    (0, 4, 6, 0, 0), (1, 4, 6, 0, 0), (0, 5, 2, 0, 0), (1, 5, 2, 1, 7), (0, 4, 7, 0, 0), (0, 5, 5, 0, 0),
    (0, 5, 13, 0, 0), (0, 5, 6, 0, 0), (1, 5, 6, 0, 0), (0, 4, 0, 0, 0), (0, 5, 7, 0, 0), (0, 5, 0, 0, 0),
)


NSLOT = len(OFFSETS)
CHUNKS = 1 + max(item[1] for item in PLAN)
OWN = OFFSETS.index((0, 0, 0))
STEPS = (
    (1, 0, 0), (3, 0, 0), (0, 1, 0), (0, 3, 0), (0, 0, 1), (0, 0, 7),
    (0, 0, 2), (0, 0, 6), (0, 0, 3), (0, 0, 5),
)
EPS_CHUNK = CHUNKS // 2
SIDES = (4, 4, 8)
MESH = pl.DeviceIdType.MESH
NI = 8
GROUP = 4
F32 = jnp.float32


def difference(first, second):
    return tuple((a - b) % side for a, b, side in zip(first, second, SIDES))


def weight_table():
    seen = set()
    table = np.zeros((NROW, 1, 128), np.float32)
    for row in range(NROW):
        for col in range(COLS):
            step = difference(OFFSETS[ROW0 + row], OFFSETS[col])
            back = difference((0, 0, 0), step)
            if min(step, back) in seen:
                continue
            seen.add(min(step, back))
            table[row, 0, col * 16 : col * 16 + 16] = 0.5 if step == back else 1.0
    assert len(seen) == 68
    return table


def kernel(
    x_ref, eps_ref, occ_ref, weight_ref, out_ref,
    raw, buf, acc, accr, epsbuf, epspart, pair_acc, square, vsrc, vrecv, csrc, crecv,
    plane, line,
    in_sem, part_send, part_recv, ring_send, ring_recv, eps_send, eps_recv,
    acc_send, acc_recv, v_send, v_recv, p_send, p_recv, l_send, l_recv,
):
    row = lax.axis_index("row")
    col = lax.axis_index("col")
    core = row % 2
    other = 1 - core
    cy = (row // 2) % 4
    cx = (col % 2) * 2 + row // 8
    cz = col // 2

    def device(step, which):
        x = (cx + step[0]) % 4
        y = (cy + step[1]) % 4
        z = (cz + step[2]) % 8
        return ((x % 2) * 8 + y * 2 + which, z * 2 + x // 2)

    partner = device((0, 0, 0), other)
    pending = []

    def send(src, dst, send_sem, recv_sem, target):
        copy = pltpu.make_async_remote_copy(
            src_ref=src, dst_ref=dst, send_sem=send_sem, recv_sem=recv_sem,
            device_id=target, device_id_type=MESH,
        )
        copy.start()
        pending.append(copy)
        return copy

    def arrived(ref, send_sem, recv_sem, target):
        pltpu.make_async_remote_copy(
            src_ref=ref, dst_ref=ref, send_sem=send_sem, recv_sem=recv_sem,
            device_id=target, device_id_type=MESH,
        ).wait_recv()

    peers = {(0, 0, 0, 1)}
    for step in {item[3] for item in PLAN if item[0] == 1}:
        peers |= {STEPS[step] + (0,), difference((0, 0, 0), STEPS[step]) + (0,)}
    barrier = pltpu.get_barrier_semaphore()
    for peer in sorted(peers):
        pl.semaphore_signal(
            barrier, inc=1, device_id=device(peer[:3], other if peer[3] else core),
            device_id_type=MESH,
        )
    pl.semaphore_wait(barrier, len(peers))

    half = x_ref.shape[1] // 2
    width = half // CHUNKS
    mine = pl.ds(pl.multiple_of(core * 64, 64), 64)
    theirs = pl.ds(pl.multiple_of(other * 64, 64), 64)
    local = pltpu.make_async_copy(
        x_ref.at[:, pl.ds(pl.multiple_of(core * half, 128), half)], raw.at[mine], in_sem
    )
    send(
        x_ref.at[:, pl.ds(pl.multiple_of(other * half, 128), half)], raw.at[mine],
        part_send.at[0], part_recv.at[0], partner,
    )
    local.start()
    send(eps_ref, epspart, part_send.at[1], part_recv.at[1], partner)

    lane = lax.broadcasted_iota(jnp.int32, (1, 128), 1)
    lane8 = lax.broadcasted_iota(jnp.int32, (8, 128), 1)
    sub8 = lax.broadcasted_iota(jnp.int32, (8, 128), 0)
    to = lax.broadcasted_iota(jnp.int32, (128, 128), 0)
    source = lax.broadcasted_iota(jnp.int32, (128, 128), 1)
    order = (source == ((to // 8) % 2) * 64 + (to % 8) * 8 + to // 16).astype(F32).astype(jnp.bfloat16)

    local.wait()
    arrived(raw.at[theirs], part_send.at[0], part_recv.at[0], partner)

    ready = set()

    def prepare(chunk):
        if chunk in ready:
            return
        ready.add(chunk)
        piece = raw[:, chunk * width : (chunk + 1) * width]
        buf[chunk, OWN] = jnp.dot(order, piece, preferred_element_type=F32).astype(jnp.bfloat16)

    def multiply(chunk, block):
        right = jnp.concatenate(
            [
                buf[chunk, 0:COLS, 16 * j : 16 * j + 16, :].reshape(COLS * 16, width)
                for j in (2 * block, 2 * block + 1)
            ],
            axis=0,
        )
        lanes = slice(256 * block, 256 * block + 256)
        for k in range(0, NROW, GROUP):
            count = min(GROUP, NROW - k)
            left = buf[chunk, ROW0 + k : ROW0 + k + count].reshape(count * 128, width)
            part = lax.dot_general(
                left, right, (((1,), (1,)), ((), ())), preferred_element_type=F32
            ).reshape(count, NI, 2, 8, 256)
            for h in range(2):
                if chunk == FIRST:
                    acc[k : k + count, h, :, :, lanes] = part[:, :, h]
                else:
                    acc[k : k + count, h, :, :, lanes] += part[:, :, h]

    def eps_exchange():
        arrived(epspart, part_send.at[1], part_recv.at[1], partner)
        epsbuf[OWN] = jnp.where((lane // 8) % 2 == core, eps_ref[...], epspart[...])

    left_in = [NSLOT - 1] * CHUNKS
    queue = []
    for kind, chunk, slot, step, target in PLAN:
        if kind == 0:
            arrived(
                buf.at[chunk, slot], ring_send.at[chunk, slot], ring_recv.at[chunk, slot], partner
            )
            if chunk == EPS_CHUNK:
                arrived(epsbuf.at[slot], eps_send.at[slot], eps_recv.at[slot], partner)
            left_in[chunk] -= 1
            if queue:
                multiply(*queue.pop(0))
            if left_in[chunk] == 0:
                queue += [(chunk, block) for block in range(4)]
        else:
            if slot == OWN:
                if chunk == EPS_CHUNK and chunk not in ready:
                    eps_exchange()
                prepare(chunk)
            send(
                buf.at[chunk, slot], buf.at[chunk, target],
                ring_send.at[chunk, target], ring_recv.at[chunk, target],
                device(STEPS[step], core),
            )
            if chunk == EPS_CHUNK:
                send(
                    epsbuf.at[slot], epsbuf.at[target], eps_send.at[target],
                    eps_recv.at[target], device(STEPS[step], core),
                )

    for chunk, block in queue:
        multiply(chunk, block)
        if chunk == LAST:
            lanes = slice(256 * block, 256 * block + 256)
            send(
                acc.at[:, other, :, :, lanes], accr.at[:, :, :, lanes],
                acc_send.at[block], acc_recv.at[block], partner,
            )

    virt_col = jnp.zeros((1, 128), F32)
    for slot in range(COLS):
        virt_col = jnp.where(lane // 16 == slot, epsbuf[slot], virt_col)
    virt_col = jnp.broadcast_to(virt_col, (8, 128))
    pair_acc[...] = jnp.zeros_like(pair_acc)
    square[...] = jnp.zeros_like(square)

    for block in range(4):
        lanes = slice(256 * block, 256 * block + 256)
        arrived(accr.at[:, :, :, lanes], acc_send.at[block], acc_recv.at[block], partner)

    def energy(k, col_sum):
        spread = jnp.broadcast_to(epsbuf[ROW0 + k], (8, 128))
        virt_row = jnp.sum(
            jnp.where(lane8 == 8 * core + sub8, spread, 0.0), axis=1, keepdims=True
        )
        virt = virt_row + virt_col
        weight = jnp.broadcast_to(weight_ref[k], (8, 128))
        total = jnp.zeros((8, 128), F32)
        count = 0
        for i in range(NI):
            for j in range(i, NI):
                here = slice(128 * j, 128 * j + 128)
                there = slice(128 * i, 128 * i + 128)
                scale = weight / ((occ_ref[i] + occ_ref[j]) - virt)
                t = acc[k, core, i, :, here] + accr[k, i, :, here]
                if i == j:
                    term = t * t * scale
                    pair_acc[count] += 2.0 * term
                else:
                    s = acc[k, core, j, :, there] + accr[k, j, :, there]
                    term = (t * (2.0 * t - s) + s * (2.0 * s - t)) * scale
                    pair_acc[count] += term
                total += term
                count += 1
        square[pl.ds(pl.multiple_of(k * 8, 8), 8), :] = total
        return col_sum + total

    col_sum = lax.fori_loop(0, NROW, energy, jnp.zeros((8, 128), F32))
    vsrc[:, 0:128] = jnp.sum(square[...].T, axis=0, keepdims=True)
    vsrc[:, 128:256] = jnp.sum(col_sum, axis=0, keepdims=True)

    here = cx * 4 + cy
    count = 0
    square[...] = jnp.zeros_like(square)
    for i in range(NI):
        for j in range(i, NI):
            total = jnp.sum(pair_acc[count], axis=0, keepdims=True)
            square[i * 8 + j : i * 8 + j + 1, :] = total
            square[j * 8 + i : j * 8 + i + 1, :] = total
            count += 1
    plane[here] = jnp.sum(square[...].T, axis=0, keepdims=True)
    for m in range(1, 16):
        send(
            plane.at[here], plane.at[here], p_send.at[m], p_recv.at[m],
            device((m // 4, m % 4, 0), core),
        )

    used = [s for s in range(NSLOT) if s != OWN and (s < COLS or ROW0 <= s < ROW0 + NROW)]
    for slot in used:
        step = difference((0, 0, 0), OFFSETS[slot])
        send(vsrc, vrecv.at[slot], v_send.at[slot], v_recv.at[slot], device(step, core))
    row_total = jnp.zeros((1, 128), F32)
    col_total = jnp.zeros((1, 128), F32)
    for slot in used + [OWN]:
        if slot == OWN:
            message = vsrc[...]
        else:
            arrived(vrecv.at[slot], v_send.at[slot], v_recv.at[slot], partner)
            message = vrecv[slot]
        if ROW0 <= slot < ROW0 + NROW:
            row_total += jnp.where(lane // 8 == slot - ROW0, message[:, 0:128], 0.0)
        if slot < COLS:
            col_total += jnp.where(lane // 16 == slot, message[:, 128:256], 0.0)
    csrc[...] = col_total
    send(csrc, crecv, part_send.at[2], part_recv.at[2], partner)

    def gathered(ref, index, send_sem, recv_sem):
        arrived(ref.at[index], send_sem, recv_sem, partner)

    for m in range(1, 16):
        x = (cx + 4 - m // 4) % 4
        y = (cy + 4 - m % 4) % 4
        gathered(plane, x * 4 + y, p_send.at[m], p_recv.at[m])
    now = cz * 2 + core
    line[now] = jnp.sum(plane[...], axis=0)
    for m in range(1, 16):
        which = core if m % 2 == 0 else other
        send(
            line.at[now], line.at[now], l_send.at[m], l_recv.at[m],
            device((0, 0, m // 2), which),
        )
    arrived(crecv, part_send.at[2], part_recv.at[2], partner)
    virt = row_total + jnp.where((lane // 8) % 2 == core, col_total + crecv[...], 0.0)

    def fold(value):
        for shift in (64, 32, 16, 8):
            value = value + pltpu.roll(value, shift, 1)
        return value

    out_ref[8:16, :] = fold(jnp.broadcast_to(virt, (8, 128)))
    for m in range(1, 16):
        z = (cz + 8 - m // 2) % 8
        which = core if m % 2 == 0 else other
        gathered(line, z * 2 + which, l_send.at[m], l_recv.at[m])
    total = jnp.broadcast_to(jnp.sum(line[...], axis=0), (8, 128))
    out_ref[0:8, :] = fold(jnp.where(lane8 // 8 == sub8, total, 0.0))
    for copy in pending:
        copy.wait_send()


def on_device(orbital_factors, occ_energy, virt_energy):
    naux = orbital_factors.shape[2]
    width = naux // 2 // CHUNKS
    eps = jnp.tile(virt_energy.astype(F32), 16).reshape(1, 128)
    vmem = pl.BlockSpec(memory_space=pltpu.VMEM)
    dma = pltpu.SemaphoreType.DMA
    out = pl.pallas_call(
        kernel,
        out_shape=jax.ShapeDtypeStruct((16, 128), F32),
        in_specs=[pl.BlockSpec(memory_space=pl.ANY), vmem, pl.BlockSpec(memory_space=pltpu.SMEM), vmem],
        out_specs=vmem,
        scratch_shapes=[
            pltpu.VMEM((128, naux // 2), jnp.bfloat16),
            pltpu.VMEM((CHUNKS, NSLOT, 128, width), jnp.bfloat16),
            pltpu.VMEM((NROW, 2, NI, 8, 1024), F32),
            pltpu.VMEM((NROW, NI, 8, 1024), F32),
            pltpu.VMEM((NSLOT, 1, 128), F32),
            pltpu.VMEM((1, 128), F32),
            pltpu.VMEM((36, 8, 128), F32),
            pltpu.VMEM((128, 128), F32),
            pltpu.VMEM((1, 256), F32),
            pltpu.VMEM((NSLOT, 1, 256), F32),
            pltpu.VMEM((1, 128), F32),
            pltpu.VMEM((1, 128), F32),
            pltpu.VMEM((16, 1, 128), F32),
            pltpu.VMEM((16, 1, 128), F32),
            dma(()),
            dma((3,)), dma((3,)),
            dma((CHUNKS, NSLOT)), dma((CHUNKS, NSLOT)),
            dma((NSLOT,)), dma((NSLOT,)),
            dma((4,)), dma((4,)),
            dma((NSLOT,)), dma((NSLOT,)),
            dma((16,)), dma((16,)),
            dma((16,)), dma((16,)),
        ],
        compiler_params=pltpu.CompilerParams(
            collective_id=0, has_side_effects=True, vmem_limit_bytes=60 * 2**20
        ),
    )(
        orbital_factors.reshape(-1, naux), eps, occ_energy.astype(F32), jnp.asarray(weight_table()),
    )
    return out[0:8, 0:8], out[8, 0:8]


def solution(mesh):
    return jax.shard_map(
        on_device,
        mesh=mesh,
        in_specs=(P(("row", "col"), None, None), P(), P(("row", "col"))),
        out_specs=(P(), P(("row", "col"))),
        check_vma=False,
    )
```

```python
import functools

import jax
import jax.numpy as jnp
import numpy as np
from jax import lax
from jax.experimental import pallas as pl
from jax.experimental.pallas import tpu as pltpu
from jax.sharding import PartitionSpec as P

OFFSETS = (
    (0, 3, 1),
    (2, 0, 1),
    (1, 3, 1),
    (3, 0, 5),
    (3, 0, 1),
    (2, 2, 1),
    (3, 2, 1),
    (0, 0, 5),
    (0, 0, 0),
    (0, 1, 6),
    (2, 3, 1),
    (0, 1, 0),
    (0, 1, 7),
    (0, 0, 7),
    (0, 0, 1),
    (0, 0, 6),
)
COLS = 8
ROW0 = 6
NROW = 10
FIRST = 0
LAST = 3
PLAN = (
    (1, 0, 8, 4, 14), (1, 0, 8, 5, 13), (1, 2, 8, 2, 11), (1, 1, 8, 4, 14), (1, 1, 8, 5, 13), (1, 3, 8, 2, 11),
    (0, 0, 13, 0, 0), (0, 0, 14, 0, 0), (1, 0, 14, 1, 4), (1, 0, 14, 3, 0), (0, 2, 11, 0, 0), (1, 0, 13, 5, 15),
    (1, 2, 8, 4, 14), (0, 1, 13, 0, 0), (0, 1, 14, 0, 0), (1, 1, 14, 1, 4), (1, 1, 14, 3, 0), (0, 3, 11, 0, 0),
    (0, 0, 0, 0, 0), (0, 0, 4, 0, 0), (1, 0, 0, 0, 2), (1, 1, 13, 5, 15), (1, 3, 8, 4, 14), (0, 0, 15, 0, 0),
    (0, 2, 14, 0, 0), (1, 0, 4, 1, 1), (1, 0, 15, 2, 9), (1, 2, 14, 3, 0), (0, 1, 0, 0, 0), (0, 1, 4, 0, 0),
    (1, 1, 0, 0, 2), (1, 2, 8, 5, 13), (0, 0, 2, 0, 0), (0, 1, 15, 0, 0), (0, 3, 14, 0, 0), (1, 1, 4, 1, 1),
    (1, 1, 15, 2, 9), (1, 3, 14, 3, 0), (0, 0, 1, 0, 0), (0, 0, 9, 0, 0), (0, 2, 0, 0, 0), (1, 0, 9, 4, 12),
    (1, 2, 0, 0, 2), (1, 0, 15, 5, 7), (0, 1, 2, 0, 0), (0, 2, 13, 0, 0), (1, 0, 1, 3, 10), (1, 3, 14, 1, 4),
    (0, 1, 1, 0, 0), (0, 1, 9, 0, 0), (0, 3, 0, 0, 0), (1, 1, 9, 4, 12), (1, 3, 0, 0, 2), (1, 3, 8, 5, 13),
    (0, 0, 12, 0, 0), (0, 2, 2, 0, 0), (0, 0, 7, 0, 0), (1, 0, 7, 1, 3), (1, 1, 1, 3, 10), (0, 0, 10, 0, 0),
    (0, 3, 4, 0, 0), (1, 0, 12, 4, 11), (1, 2, 2, 0, 10), (1, 2, 13, 5, 15), (0, 1, 12, 0, 0), (0, 3, 2, 0, 0),
    (0, 3, 13, 0, 0), (1, 0, 10, 3, 5), (1, 2, 14, 1, 4), (0, 0, 3, 0, 0), (0, 1, 10, 0, 0), (1, 1, 12, 4, 11),
    (1, 3, 2, 0, 10), (1, 1, 15, 5, 7), (0, 0, 11, 0, 0), (0, 2, 10, 0, 0), (1, 2, 10, 2, 1), (0, 2, 15, 0, 0),
    (1, 1, 10, 3, 5), (1, 3, 4, 1, 1), (0, 0, 5, 0, 0), (0, 2, 4, 0, 0), (1, 0, 5, 0, 6), (1, 3, 13, 5, 15),
    (0, 1, 11, 0, 0), (0, 3, 10, 0, 0), (1, 2, 15, 2, 9), (0, 1, 7, 0, 0), (1, 1, 7, 1, 3), (1, 2, 10, 3, 5),
    (0, 2, 1, 0, 0), (0, 1, 5, 0, 0), (0, 3, 1, 0, 0), (1, 1, 5, 0, 6), (1, 2, 15, 5, 7), (0, 0, 6, 0, 0),
    (0, 3, 15, 0, 0), (1, 3, 10, 3, 5), (1, 3, 15, 2, 9), (0, 2, 9, 0, 0), (1, 2, 9, 4, 12), (0, 1, 3, 0, 0),
    (0, 2, 5, 0, 0), (1, 2, 5, 0, 6), (1, 3, 15, 5, 7), (0, 1, 6, 0, 0), (0, 2, 7, 0, 0), (1, 2, 7, 1, 3),
    (0, 3, 5, 0, 0), (0, 3, 9, 0, 0), (1, 3, 5, 0, 6), (1, 3, 11, 5, 12), (0, 2, 12, 0, 0), (0, 2, 6, 0, 0),
    (0, 3, 7, 0, 0), (1, 3, 7, 1, 3), (0, 2, 3, 0, 0), (0, 3, 6, 0, 0), (0, 3, 12, 0, 0), (0, 3, 3, 0, 0),
)


NSLOT = len(OFFSETS)
CHUNKS = 1 + max(item[1] for item in PLAN)
OWN = OFFSETS.index((0, 0, 0))
STEPS = (
    (1, 0, 0), (3, 0, 0), (0, 1, 0), (0, 3, 0), (0, 0, 1), (0, 0, 7),
    (0, 0, 2), (0, 0, 6), (0, 0, 3), (0, 0, 5),
)
EPS_CHUNK = CHUNKS // 2
SIDES = (4, 4, 8)
MESH = pl.DeviceIdType.MESH
NI = 8
GROUP = 4
F32 = jnp.float32


def difference(first, second):
    return tuple((a - b) % side for a, b, side in zip(first, second, SIDES))


def weight_table():
    seen = set()
    table = np.zeros((NROW, 1, 128), np.float32)
    for row in range(NROW):
        for col in range(COLS):
            step = difference(OFFSETS[ROW0 + row], OFFSETS[col])
            back = difference((0, 0, 0), step)
            if min(step, back) in seen:
                continue
            seen.add(min(step, back))
            table[row, 0, col * 16 : col * 16 + 16] = 0.5 if step == back else 1.0
    assert len(seen) == 68
    return table


def kernel(
    x_ref, eps_ref, occ_ref, weight_ref, pair_ref, virt_ref,
    raw, buf, acc, accr, epsbuf, epspart, pair_acc, square, vsrc, vrecv, csrc, crecv,
    plane, line,
    in_sem, part_send, part_recv, ring_send, ring_recv, eps_send, eps_recv,
    acc_send, acc_recv, v_send, v_recv, p_send, p_recv, l_send, l_recv,
):
    row = lax.axis_index("row")
    col = lax.axis_index("col")
    core = row % 2
    other = 1 - core
    cy = (row // 2) % 4
    cx = (col % 2) * 2 + row // 8
    cz = col // 2

    def device(step, which):
        x = (cx + step[0]) % 4
        y = (cy + step[1]) % 4
        z = (cz + step[2]) % 8
        return ((x % 2) * 8 + y * 2 + which, z * 2 + x // 2)

    partner = device((0, 0, 0), other)
    pending = []

    def send(src, dst, send_sem, recv_sem, target):
        copy = pltpu.make_async_remote_copy(
            src_ref=src, dst_ref=dst, send_sem=send_sem, recv_sem=recv_sem,
            device_id=target, device_id_type=MESH,
        )
        copy.start()
        pending.append(copy)
        return copy

    def arrived(ref, send_sem, recv_sem, target):
        pltpu.make_async_remote_copy(
            src_ref=ref, dst_ref=ref, send_sem=send_sem, recv_sem=recv_sem,
            device_id=target, device_id_type=MESH,
        ).wait_recv()

    peers = {(0, 0, 0, 1)}
    for step in {item[3] for item in PLAN if item[0] == 1}:
        peers |= {STEPS[step] + (0,), difference((0, 0, 0), STEPS[step]) + (0,)}
    barrier = pltpu.get_barrier_semaphore()
    for peer in sorted(peers):
        pl.semaphore_signal(
            barrier, inc=1, device_id=device(peer[:3], other if peer[3] else core),
            device_id_type=MESH,
        )
    pl.semaphore_wait(barrier, len(peers))

    half = x_ref.shape[1] // 2
    width = half // CHUNKS
    mine = pl.ds(pl.multiple_of(core * 64, 64), 64)
    theirs = pl.ds(pl.multiple_of(other * 64, 64), 64)
    parts = ((0, width), (width, half - width))
    for index, (start, size) in enumerate(parts):
        send(
            x_ref.at[:, pl.ds(pl.multiple_of(other * half + start, 128), size)],
            raw.at[mine, pl.ds(start, size)],
            part_send.at[3 * index], part_recv.at[3 * index], partner,
        )
    local = [
        pltpu.make_async_copy(
            x_ref.at[:, pl.ds(pl.multiple_of(core * half + start, 128), size)],
            raw.at[mine, pl.ds(start, size)],
            in_sem.at[index],
        )
        for index, (start, size) in enumerate(parts)
    ]
    for copy in local:
        copy.start()
    send(eps_ref, epspart, part_send.at[1], part_recv.at[1], partner)

    lane = lax.broadcasted_iota(jnp.int32, (1, 128), 1)
    lane8 = lax.broadcasted_iota(jnp.int32, (8, 128), 1)
    sub8 = lax.broadcasted_iota(jnp.int32, (8, 128), 0)
    to = lax.broadcasted_iota(jnp.int32, (128, 128), 0)
    source = lax.broadcasted_iota(jnp.int32, (128, 128), 1)
    order = (source == ((to // 8) % 2) * 64 + (to % 8) * 8 + to // 16).astype(F32).astype(jnp.bfloat16)

    def take(index):
        start, size = parts[index]
        local[index].wait()
        arrived(
            raw.at[theirs, pl.ds(start, size)], part_send.at[3 * index], part_recv.at[3 * index],
            partner,
        )

    ready = set()

    def prepare(chunk):
        if chunk in ready:
            return
        if len(ready) < 2:
            take(len(ready))
        assert ready or chunk == 0
        ready.add(chunk)
        piece = raw[:, chunk * width : (chunk + 1) * width]
        buf[chunk, OWN] = jnp.dot(order, piece, preferred_element_type=F32).astype(jnp.bfloat16)

    def multiply(chunk, block, groups):
        right = jnp.concatenate(
            [
                buf[chunk, 0:COLS, 16 * j : 16 * j + 16, :].reshape(COLS * 16, width)
                for j in (2 * block, 2 * block + 1)
            ],
            axis=0,
        )
        lanes = slice(256 * block, 256 * block + 256)
        for k, count in groups:
            left = buf[chunk, ROW0 + k : ROW0 + k + count].reshape(count * 128, width)
            part = lax.dot_general(
                left, right, (((1,), (1,)), ((), ())), preferred_element_type=F32
            ).reshape(count, NI, 2, 8, 256)
            for h in range(2):
                if chunk == FIRST:
                    acc[k : k + count, h, :, :, lanes] = part[:, :, h]
                else:
                    acc[k : k + count, h, :, :, lanes] += part[:, :, h]

    groups = [(k, min(GROUP, NROW - k)) for k in range(0, NROW, GROUP)]

    def eps_exchange():
        arrived(epspart, part_send.at[1], part_recv.at[1], partner)
        epsbuf[OWN] = jnp.where((lane // 8) % 2 == core, eps_ref[...], epspart[...])

    left_in = [NSLOT - 1] * CHUNKS
    queue = []
    for kind, chunk, slot, step, target in PLAN:
        if kind == 0:
            arrived(
                buf.at[chunk, slot], ring_send.at[chunk, slot], ring_recv.at[chunk, slot], partner
            )
            if chunk == EPS_CHUNK:
                arrived(epsbuf.at[slot], eps_send.at[slot], eps_recv.at[slot], partner)
            left_in[chunk] -= 1
            if queue:
                multiply(*queue.pop(0), groups)
            if left_in[chunk] == 0:
                queue += [(chunk, block) for block in range(4)]
        else:
            if slot == OWN:
                if chunk == EPS_CHUNK and chunk not in ready:
                    eps_exchange()
                prepare(chunk)
            send(
                buf.at[chunk, slot], buf.at[chunk, target],
                ring_send.at[chunk, target], ring_recv.at[chunk, target],
                device(STEPS[step], core),
            )
            if chunk == EPS_CHUNK:
                send(
                    epsbuf.at[slot], epsbuf.at[target], eps_send.at[target],
                    eps_recv.at[target], device(STEPS[step], core),
                )

    for chunk, block in queue:
        if chunk != LAST:
            multiply(chunk, block, groups)
    for index, (k, count) in enumerate(groups):
        for block in range(4):
            multiply(LAST, block, [(k, count)])
        send(
            acc.at[k : k + count, other], accr.at[k : k + count],
            acc_send.at[index], acc_recv.at[index], partner,
        )

    virt_col = jnp.zeros((1, 128), F32)
    for slot in range(COLS):
        virt_col = jnp.where(lane // 16 == slot, epsbuf[slot], virt_col)
    virt_col = jnp.broadcast_to(virt_col, (8, 128))
    pair_acc[...] = jnp.zeros_like(pair_acc)
    square[...] = jnp.zeros_like(square)

    def energy(k, col_sum):
        spread = jnp.broadcast_to(epsbuf[ROW0 + k], (8, 128))
        virt_row = jnp.sum(
            jnp.where(lane8 == 8 * core + sub8, spread, 0.0), axis=1, keepdims=True
        )
        virt = virt_row + virt_col
        weight = jnp.broadcast_to(weight_ref[k], (8, 128))
        total = jnp.zeros((8, 128), F32)
        count = 0
        for i in range(NI):
            for j in range(i, NI):
                here = slice(128 * j, 128 * j + 128)
                there = slice(128 * i, 128 * i + 128)
                scale = weight / ((occ_ref[i] + occ_ref[j]) - virt)
                t = acc[k, core, i, :, here] + accr[k, i, :, here]
                if i == j:
                    term = t * t * scale
                    pair_acc[count] += 2.0 * term
                else:
                    s = acc[k, core, j, :, there] + accr[k, j, :, there]
                    term = (t * (2.0 * t - s) + s * (2.0 * s - t)) * scale
                    pair_acc[count] += term
                total += term
                count += 1
        square[pl.ds(pl.multiple_of(k * 8, 8), 8), :] = total
        return col_sum + total

    col_sum = jnp.zeros((8, 128), F32)
    for index, (k, count) in enumerate(groups):
        arrived(accr.at[k : k + count], acc_send.at[index], acc_recv.at[index], partner)
        col_sum = lax.fori_loop(k, k + count, energy, col_sum)
    vsrc[:, 0:128] = jnp.sum(square[...].T, axis=0, keepdims=True)
    vsrc[:, 128:256] = jnp.sum(col_sum, axis=0, keepdims=True)

    here = cx * 4 + cy
    count = 0
    square[...] = jnp.zeros_like(square)
    for i in range(NI):
        for j in range(i, NI):
            total = jnp.sum(pair_acc[count], axis=0, keepdims=True)
            square[i * 8 + j : i * 8 + j + 1, :] = total
            square[j * 8 + i : j * 8 + i + 1, :] = total
            count += 1
    plane[here] = jnp.sum(square[...].T, axis=0, keepdims=True)
    for m in range(1, 16):
        send(
            plane.at[here], plane.at[here], p_send.at[m], p_recv.at[m],
            device((m // 4, m % 4, 0), core),
        )

    used = [s for s in range(NSLOT) if s != OWN and (s < COLS or ROW0 <= s < ROW0 + NROW)]
    for slot in used:
        step = difference((0, 0, 0), OFFSETS[slot])
        send(vsrc, vrecv.at[slot], v_send.at[slot], v_recv.at[slot], device(step, core))
    row_total = jnp.zeros((1, 128), F32)
    col_total = jnp.zeros((1, 128), F32)
    for slot in used + [OWN]:
        if slot == OWN:
            message = vsrc[...]
        else:
            arrived(vrecv.at[slot], v_send.at[slot], v_recv.at[slot], partner)
            message = vrecv[slot]
        if ROW0 <= slot < ROW0 + NROW:
            row_total += jnp.where(lane // 8 == slot - ROW0, message[:, 0:128], 0.0)
        if slot < COLS:
            col_total += jnp.where(lane // 16 == slot, message[:, 128:256], 0.0)
    csrc[...] = col_total
    send(csrc, crecv, part_send.at[2], part_recv.at[2], partner)

    def gathered(ref, index, send_sem, recv_sem):
        arrived(ref.at[index], send_sem, recv_sem, partner)

    for m in range(1, 16):
        x = (cx + 4 - m // 4) % 4
        y = (cy + 4 - m % 4) % 4
        gathered(plane, x * 4 + y, p_send.at[m], p_recv.at[m])
    now = cz * 2 + core
    line[now] = jnp.sum(plane[...], axis=0)
    for m in range(1, 16):
        which = core if m % 2 == 0 else other
        send(
            line.at[now], line.at[now], l_send.at[m], l_recv.at[m],
            device((0, 0, m // 2), which),
        )
    arrived(crecv, part_send.at[2], part_recv.at[2], partner)
    virt = row_total + jnp.where((lane // 8) % 2 == core, col_total + crecv[...], 0.0)

    def fold(value):
        for shift in (64, 32, 16, 8):
            value = value + pltpu.roll(value, shift, 1)
        return value

    virt_ref[...] = fold(jnp.broadcast_to(virt, (8, 128)))[0:1, 0:8]
    for m in range(1, 16):
        z = (cz + 8 - m // 2) % 8
        which = core if m % 2 == 0 else other
        gathered(line, z * 2 + which, l_send.at[m], l_recv.at[m])
    total = jnp.broadcast_to(jnp.sum(line[...], axis=0), (8, 128))
    pair_ref[...] = fold(jnp.where(lane8 // 8 == sub8, total, 0.0))[:, 0:8]
    for copy in pending:
        copy.wait_send()


def on_device(orbital_factors, occ_energy, virt_energy):
    naux = orbital_factors.shape[2]
    width = naux // 2 // CHUNKS
    eps = jnp.tile(virt_energy.astype(F32), 16).reshape(1, 128)
    vmem = pl.BlockSpec(memory_space=pltpu.VMEM)
    dma = pltpu.SemaphoreType.DMA
    pair, virt = pl.pallas_call(
        kernel,
        out_shape=[jax.ShapeDtypeStruct((8, 8), F32), jax.ShapeDtypeStruct((1, 8), F32)],
        in_specs=[pl.BlockSpec(memory_space=pl.ANY), vmem, pl.BlockSpec(memory_space=pltpu.SMEM), vmem],
        out_specs=[vmem, vmem],
        scratch_shapes=[
            pltpu.VMEM((128, naux // 2), jnp.bfloat16),
            pltpu.VMEM((CHUNKS, NSLOT, 128, width), jnp.bfloat16),
            pltpu.VMEM((NROW, 2, NI, 8, 1024), F32),
            pltpu.VMEM((NROW, NI, 8, 1024), F32),
            pltpu.VMEM((NSLOT, 1, 128), F32),
            pltpu.VMEM((1, 128), F32),
            pltpu.VMEM((36, 8, 128), F32),
            pltpu.VMEM((128, 128), F32),
            pltpu.VMEM((1, 256), F32),
            pltpu.VMEM((NSLOT, 1, 256), F32),
            pltpu.VMEM((1, 128), F32),
            pltpu.VMEM((1, 128), F32),
            pltpu.VMEM((16, 1, 128), F32),
            pltpu.VMEM((16, 1, 128), F32),
            dma((2,)),
            dma((4,)), dma((4,)),
            dma((CHUNKS, NSLOT)), dma((CHUNKS, NSLOT)),
            dma((NSLOT,)), dma((NSLOT,)),
            dma((4,)), dma((4,)),
            dma((NSLOT,)), dma((NSLOT,)),
            dma((16,)), dma((16,)),
            dma((16,)), dma((16,)),
        ],
        compiler_params=pltpu.CompilerParams(
            collective_id=0, has_side_effects=True, vmem_limit_bytes=60 * 2**20
        ),
    )(
        orbital_factors.reshape(-1, naux), eps, occ_energy.astype(F32), jnp.asarray(weight_table()),
    )
    return pair, virt.reshape(8)


def solution(mesh):
    return jax.shard_map(
        on_device,
        mesh=mesh,
        in_specs=(P(("row", "col"), None, None), P(), P(("row", "col"))),
        out_specs=(P(), P(("row", "col"))),
        check_vma=False,
    )
```
